32 devices in a mesh: batch: 1 (over z), seq: 32 (over y, x, core).
Axes of the slice: x: 4, y: 4, z: 1, core: 2. Of those that a mesh axis runs over, the one named last changes fastest.
The devices are a block of a 4x4x8 slice.
Arguments:
- hidden: bfloat16 [32, 4, 7168], P('batch')
- cache_lens: int32 [32], P('batch')
- c_kv: bfloat16 [32, 32768, 512], P('batch', 'seq')
- k_r: bfloat16 [32, 32768, 64], P('batch', 'seq')
- w_uq: bfloat16 [7168, 64, 128], P(None, 'seq')
- w_qr: bfloat16 [7168, 64, 64], P(None, 'seq')
- w_uk: bfloat16 [64, 128, 512], P('seq')
- w_uv: bfloat16 [64, 512, 128], P('seq')
- w_o: bfloat16 [64, 128, 7168], P('seq')
Outputs:
- output: bfloat16 [32, 4, 7168], P('batch')
All inputs are finite; a program needn't handle non-finite values.
Results may differ from the reference program's by a relative error of at most 0.00646674.
Values are sent between devices in bfloat16 or wider.
A program may use at most 768 MiB of HBM per device.

```python
import jax
import jax.numpy as jnp
from jax import lax

ROW_COUNT = 32
CTX_LEN = 32768
Q_LEN = 4
MODEL_DIM = 7168
NUM_HEADS = 64
NOPE_DIM = 128
ROPE_DIM = 64
LATENT_DIM = 512
VALUE_DIM = 128


def setup_inputs(seed: int = 0, part: int = 0) -> dict:
    part_key = jax.random.fold_in(jax.random.key(seed), part)
    key_x, key_lens, key_cache, key_rope = jax.random.split(part_key, 4)
    key_uq, key_qr, key_uk, key_uv, key_wo = jax.random.split(jax.random.key(seed + 1), 5)
    hidden = jax.random.normal(key_x, (ROW_COUNT, Q_LEN, MODEL_DIM), jnp.float32)
    short_by = jax.random.randint(key_lens, (ROW_COUNT,), 0, CTX_LEN // 4 + 1)
    cache_lens = (CTX_LEN - Q_LEN - short_by).at[0].set(CTX_LEN - Q_LEN)
    c_kv = jax.random.normal(key_cache, (ROW_COUNT, CTX_LEN, LATENT_DIM), jnp.float32)
    k_r = jax.random.normal(key_rope, (ROW_COUNT, CTX_LEN, ROPE_DIM), jnp.float32)
    w_uq = jax.random.normal(key_uq, (MODEL_DIM, NUM_HEADS, NOPE_DIM), jnp.float32) * MODEL_DIM ** -0.5
    w_qr = jax.random.normal(key_qr, (MODEL_DIM, NUM_HEADS, ROPE_DIM), jnp.float32) * (2.0 * MODEL_DIM ** -0.5)
    w_uk = jax.random.normal(key_uk, (NUM_HEADS, NOPE_DIM, LATENT_DIM), jnp.float32) * (2.0 * NOPE_DIM ** -0.5)
    w_uv = jax.random.normal(key_uv, (NUM_HEADS, LATENT_DIM, VALUE_DIM), jnp.float32) * LATENT_DIM ** -0.5
    w_o = jax.random.normal(key_wo, (NUM_HEADS, VALUE_DIM, MODEL_DIM), jnp.float32) * (2.0 * (NUM_HEADS * VALUE_DIM) ** -0.5)
    return {
        "hidden": hidden.astype(jnp.bfloat16),
        "cache_lens": cache_lens.astype(jnp.int32),
        "c_kv": c_kv.astype(jnp.bfloat16),
        "k_r": k_r.astype(jnp.bfloat16),
        "w_uq": w_uq.astype(jnp.bfloat16),
        "w_qr": w_qr.astype(jnp.bfloat16),
        "w_uk": w_uk.astype(jnp.bfloat16),
        "w_uv": w_uv.astype(jnp.bfloat16),
        "w_o": w_o.astype(jnp.bfloat16),
    }


def reference(hidden, cache_lens, c_kv, k_r, w_uq, w_qr, w_uk, w_uv, w_o):
    hidden_wide = hidden.astype(jnp.float32)
    q_nope = jnp.einsum("bqd,dhk->bqhk", hidden_wide, w_uq.astype(jnp.float32)).astype(jnp.bfloat16)
    q_rope = jnp.einsum("bqd,dhr->bqhr", hidden_wide, w_qr.astype(jnp.float32)).astype(jnp.bfloat16)
    q_lat = jnp.einsum("bqhk,hkc->bqhc", q_nope.astype(jnp.float32), w_uk.astype(jnp.float32)).astype(jnp.bfloat16)
    score_scale = (NOPE_DIM + ROPE_DIM) ** -0.5
    positions = jnp.arange(CTX_LEN)
    offsets = jnp.arange(Q_LEN)

    def row_attend(row_args):
        lat_row, rope_row, cache_row, key_row, row_len = row_args
        cache_wide = cache_row.astype(jnp.float32)
        scores = (jnp.einsum("qhc,tc->qht", lat_row.astype(jnp.float32), cache_wide)
                  + jnp.einsum("qhr,tr->qht", rope_row.astype(jnp.float32), key_row.astype(jnp.float32))) * score_scale
        visible = positions[None, None, :] <= (row_len + offsets)[:, None, None]
        probs = jax.nn.softmax(jnp.where(visible, scores, -jnp.inf), axis=-1)
        return jnp.einsum("qht,tc->qhc", probs, cache_wide)

    o_lat = lax.map(row_attend, (q_lat, q_rope, c_kv, k_r, cache_lens)).astype(jnp.bfloat16)
    o_val = jnp.einsum("bqhc,hcv->bqhv", o_lat.astype(jnp.float32), w_uv.astype(jnp.float32)).astype(jnp.bfloat16)
    y_sum = jnp.einsum("bqhv,hvd->bqd", o_val.astype(jnp.float32), w_o.astype(jnp.float32))
    return (hidden_wide + y_sum).astype(jnp.bfloat16)
```

```python
import functools
import math

import jax
import jax.numpy as jnp
from jax import lax
from jax.experimental import pallas as pl
from jax.experimental.pallas import tpu as pltpu
from jax.sharding import PartitionSpec as P

MESH = pl.DeviceIdType.MESH
F32, BF16 = jnp.float32, jnp.bfloat16
FILL = float(jnp.finfo(jnp.float32).min)
CORES = 2
VMEM_BYTES = 67_043_328


class Place:
    def __init__(self, side):
        me = lax.axis_index("seq")
        self.side = side
        self.core = lax.rem(me, CORES)
        chip = me // CORES
        self.x, self.y = lax.rem(chip, side), chip // side
        self.first, self.second = (self.x, self.y), (self.y, self.x)

    def wrap(self, i):
        return lax.rem(i + self.side, self.side)

    def yx(self, plane, f, s):
        return (s, f) if plane == 0 else (f, s)

    def device(self, plane, f, s, core=None):
        y, x = self.yx(plane, f, s)
        return (y * self.side + x) * CORES + (self.core if core is None else core)

    def sibling(self):
        return self.device(0, self.x, self.y, 1 - self.core)

    def along_first(self, plane, step):
        return self.device(plane, self.wrap(self.first[plane] + step), self.second[plane])

    def along_second(self, plane, step):
        return self.device(plane, self.first[plane], self.wrap(self.second[plane] + step))

    def barrier(self):
        barrier = pltpu.get_barrier_semaphore()
        peers = [self.sibling()] + [self.along_first(p, d) for p in range(2) for d in (1, -1)]
        for peer in peers:
            pl.semaphore_signal(barrier, inc=1, device_id={"seq": peer}, device_id_type=MESH)
        pl.semaphore_wait(barrier, len(peers))


def remote(src, dst, send, recv, device):
    return pltpu.make_async_remote_copy(src_ref=src, dst_ref=dst, send_sem=send, recv_sem=recv, device_id={"seq": device},
                                        device_id_type=MESH)


GATHER_MSGS = 12


class Gather:
    def __init__(self, place, plane, view, own, send, recv):
        self.place, self.plane, self.view, self.own, self.send, self.recv = place, plane, view, own, send, recv

    def copy(self, msg, arriving=False):
        pc, p = self.place, self.plane
        f, s, c = pc.first[p], pc.second[p], pc.core
        w = pc.wrap
        sent, got, target = {
            0: ((None, f, s), (None, w(f - 1), s), pc.along_first(p, 1)),
            1: ((None, f, s), (None, w(f + 1), s), pc.along_first(p, -1)),
            2: ((0, w(f - 1), s), (0, w(f - 2), s), pc.along_first(p, 1)),
            3: ((1, w(f + 1), s), (1, w(f + 2), s), pc.along_first(p, -1)),
            4: ((None, None, s), (None, None, w(s - 1)), pc.along_second(p, 1)),
            5: ((None, None, s), (None, None, w(s + 1)), pc.along_second(p, -1)),
            6: ((0, None, w(s - 1)), (0, None, w(s - 2)), pc.along_second(p, 1)),
            7: ((1, None, w(s + 1)), (1, None, w(s + 2)), pc.along_second(p, -1)),
            8: ((None, None, s),) * 2 + (pc.sibling(),),
            9: ((None, None, w(s - 1)),) * 2 + (pc.sibling(),),
            10: ((None, None, w(s + 1)),) * 2 + (pc.sibling(),),
            11: ((None, None, w(s + 2)),) * 2 + (pc.sibling(),),
        }[msg]
        if arriving:
            dst = self.view(1 - c if msg >= 8 else c, *got)
            src = dst
        else:
            dst = self.view(c, *sent)
            src = self.own if msg in (0, 1) else dst
        return remote(src, dst, self.send(msg), self.recv(msg), target)

    def start(self, *msgs):
        for msg in msgs:
            self.copy(msg).start()

    def wait(self, *msgs):
        for msg in msgs:
            self.copy(msg, arriving=True).wait_recv()

    def step(self, i):
        if i == 1:
            self.start(0, 1)
        elif i == 2:
            self.wait(0)
            self.start(2)
            self.wait(1)
            self.start(3)
        elif i == 3:
            self.wait(2, 3)
            self.start(4, 5, 8)
        elif i == 4:
            self.wait(4)
            self.start(6, 9)
            self.wait(5)
            self.start(7, 10)
        elif i == 5:
            self.wait(6, 7)
            self.start(11)
        elif i == 6:
            self.wait(8, 9, 10, 11)

    def drain(self):
        for msg in range(GATHER_MSGS):
            self.copy(msg).wait_send()


SCATTER_MSGS = 8


class Scatter:
    def __init__(self, place, plane, view, landing, merge, extra, send, recv):
        self.place, self.plane, self.view, self.landing = place, plane, view, landing
        self.merge, self.extra, self.send, self.recv = merge, extra, send, recv

    def plan(self, msg):
        pc, p = self.place, self.plane
        f, s = pc.first[p], pc.second[p]
        w = pc.wrap
        return {
            0: ((0, w(f + 2), None), pc.along_first(p, 1), (0, w(f + 1), None)),
            1: ((1, w(f + 2), None), pc.along_first(p, -1), (1, w(f - 1), None)),
            2: ((None, w(f + 1), None), pc.along_first(p, 1), (None, f, None)),
            3: ((None, w(f - 1), None), pc.along_first(p, -1), (None, f, None)),
            4: ((0, f, w(s + 2)), pc.along_second(p, 1), (0, f, w(s + 1))),
            5: ((1, f, w(s + 2)), pc.along_second(p, -1), (1, f, w(s - 1))),
            6: ((None, f, w(s + 1)), pc.along_second(p, 1), (None, f, s)),
            7: ((None, f, w(s - 1)), pc.along_second(p, -1), (None, f, s)),
        }[msg]

    def copies(self, msg, arriving=False):
        sent, target, _ = self.plan(msg)
        dst = self.landing(msg)
        out = [remote(dst if arriving else self.view(*sent), dst, self.send(msg), self.recv(msg), target)]
        extra = self.extra(msg)
        if extra is not None:
            src, dst = extra
            i = msg + SCATTER_MSGS
            out.append(remote(dst if arriving else src, dst, self.send(i), self.recv(i), target))
        return out

    def start(self, *msgs):
        for msg in msgs:
            for copy in self.copies(msg):
                copy.start()

    def take(self, msg):
        for copy in self.copies(msg, arriving=True):
            copy.wait_recv()
        self.merge(*self.plan(msg)[2], msg)

    def drain(self):
        for msg in range(SCATTER_MSGS):
            for copy in self.copies(msg):
                copy.wait_send()


def attention_kernel(cfg, lens_ref, q_ref, ckv_ref, krt_ref, o_ref, qall, obuf, cbuf, kbuf, stat, xt, tcur, tsend, tland, tpair,
                     factor, pair_land, far1, near1, far2, near2, gsend, grecv, ssend, srecv, psend, precv, csem, ksem):
    side, chunk, q_len, scale = cfg
    place = Place(side)
    core = place.core
    batch, lat = ckv_ref.shape[0], ckv_ref.shape[2]
    rope, local_len = krt_ref.shape[1], krt_ref.shape[2]
    block = q_ref.shape[1]
    rows = CORES * side * side * block
    lanes = side * side * block
    pairs = chunk // 2
    n_chunks = batch // chunk
    part = chunk // 2
    half = part // 2
    n_pairs = batch // 2

    def cache_copies(p, e):
        slot = lax.rem(p, 2) * 2 + e
        row = p * 2 + e
        return (pltpu.make_async_copy(ckv_ref.at[row], cbuf.at[slot], csem.at[slot]),
                pltpu.make_async_copy(krt_ref.at[row], kbuf.at[slot, pl.ds(e * rope, rope)], ksem.at[slot]))

    def fetch(p):
        for e in range(2):
            for copy in cache_copies(p, e):
                copy.start()

    for e in range(2):
        for i in range(2):
            kbuf[i * 2 + e, pl.ds((1 - e) * rope, rope)] = jnp.zeros((rope, local_len), BF16)
    fetch(0)
    fetch(1)

    for p in range(n_pairs):
        qall[p, core, place.y, place.x] = q_ref[p]
    stat[...] = jnp.zeros_like(stat)
    place.barrier()

    def gather(k, plane):
        base = k * pairs + plane * (pairs // 2)

        def view(c, h, f, s):
            if h is None:
                at = pl.ds(base, pairs // 2)
            else:
                at = pl.ds(base + h * (pairs // 4), pairs // 4)
            f = pl.ds(0, side) if f is None else f
            y, x = place.yx(plane, f, s)
            return qall.at[at, c, y, x]

        return Gather(place, plane, view, q_ref.at[pl.ds(base, pairs // 2)], lambda m: gsend.at[k, plane, m],
                      lambda m: grecv.at[k, plane, m])

    def merge_tables(ta, tb):
        m = jnp.maximum(ta, tb)
        ea, eb = jnp.exp2(ta - m), jnp.exp2(tb - m)
        top = lax.broadcasted_iota(jnp.int32, ta.shape, 0) < part
        joined = jnp.where(top, m, ta * pltpu.roll(ea, part, 0) + tb * pltpu.roll(eb, part, 0))
        factor[:, 0:4 * part] = jnp.concatenate([ea, eb], 0).T
        return joined

    def scatter(k, plane):
        base = k * chunk + plane * part

        def span(h):
            return (0, part) if h is None else (h * half, half)

        def view(h, f, s):
            lo, n = span(h)
            s = pl.ds(0, side) if s is None else s
            y, x = place.yx(plane, f, s)
            return obuf.at[pl.ds(base + lo, n), core, y, x]

        def landing(msg):
            return {0: far1, 1: near1, 2: far2, 3: near2}[msg // 2].at[k, plane, msg % 2]

        def extra(msg):
            return tsend.at[k, plane, msg], tland.at[k, plane, msg]

        def merge(h, f, s, msg):
            lo, n = span(h)
            ta = tcur[k, plane]
            joined = merge_tables(ta, tland[k, plane, msg])
            spots = lax.broadcasted_iota(jnp.int32, ta.shape, 1) // block
            ys, xs = spots // side, lax.rem(spots, side)
            fs, ss = (xs, ys) if plane == 0 else (ys, xs)
            mine = fs == f
            if s is not None:
                mine = mine & (ss == s)
            if h is not None:
                b = lax.rem(lax.broadcasted_iota(jnp.int32, ta.shape, 0), part)
                mine = mine & (b >= lo) & (b < lo + n)
            tcur[k, plane] = jnp.where(mine, joined, ta)
            land = landing(msg)
            for j in range(n):
                for i in range(side if s is None else 1):
                    y, x = place.yx(plane, f, i if s is None else s)
                    at = pl.ds(pl.multiple_of((y * side + x) * block, block), block)
                    fa = factor[at, lo + j:lo + j + 1]
                    fb = factor[at, 2 * part + lo + j:2 * part + lo + j + 1]
                    there = land[j, i] if s is None else land[j]
                    obuf[base + lo + j, core, y, x] = obuf[base + lo + j, core, y, x] * fa + there * fb

        return Scatter(place, plane, view, landing, merge, extra, lambda m: ssend.at[k, plane, m],
                       lambda m: srecv.at[k, plane, m])

    def both(make, k, act):
        for plane in range(2):
            act(make(k, plane))

    def snap(sc, k, *msgs):
        for msg in msgs:
            tsend[k, sc.plane, msg] = tcur[k, sc.plane]
        sc.start(*msgs)

    def pair_copies(k, arriving=False):
        there = pair_land.at[k]
        src = there if arriving else obuf.at[pl.ds(k * chunk, chunk), 1 - core]
        tables = tpair.at[k]
        tsrc = tables if arriving else xt.at[k, 1 - core]
        return (remote(src, there, psend.at[k, 0], precv.at[k, 0], place.sibling()),
                remote(tsrc, tables, psend.at[k, 1], precv.at[k, 1], place.sibling()))

    def pair_start(k):
        t = stat[...].T
        for c in range(CORES):
            for plane in range(2):
                xt[k, c, plane] = t[plane * 2 * part:(plane + 1) * 2 * part, c * lanes:(c + 1) * lanes]
        for copy in pair_copies(k):
            copy.start()

    def pair_merge(k):
        for copy in pair_copies(k, arriving=True):
            copy.wait_recv()
        for plane in range(2):
            tcur[k, plane] = merge_tables(xt[k, core, plane], tpair[k, plane])
            base = k * chunk + plane * part

            def spot(i, carry):
                y, x = i // side, lax.rem(i, side)
                at = pl.ds(pl.multiple_of(i * block, block), block)
                for j in range(part):
                    fa, fb = factor[at, j:j + 1], factor[at, 2 * part + j:2 * part + j + 1]
                    obuf[base + j, core, y, x] = (obuf[base + j, core, y, x] * fa
                                                  + pair_land[k, plane * part + j, y, x] * fb)
                return carry

            lax.fori_loop(0, side * side, spot, 0)

    def scatter_step(k, i):
        if i == 0:
            pair_merge(k)
            both(scatter, k, lambda sc: snap(sc, k, 0, 1))
        elif i == 1:
            for msg in (0, 1):
                both(scatter, k, lambda sc: (sc.take(msg), snap(sc, k, msg + 2)))
        elif i == 2:
            both(scatter, k, lambda sc: (sc.take(2), sc.take(3), snap(sc, k, 4, 5)))
        elif i == 3:
            for msg in (4, 5):
                both(scatter, k, lambda sc: (sc.take(msg), snap(sc, k, msg + 2)))
        elif i == 4:
            both(scatter, k, lambda sc: (sc.take(6), sc.take(7)))
            at = pl.ds(pl.multiple_of((place.y * side + place.x) * block, block), block)
            for plane in range(2):
                factor[:, 0:2 * part] = tcur[k, plane].T
                for j in range(part):
                    b = k * chunk + plane * part + j
                    o_ref[b] = (obuf[b, core, place.y, place.x] / factor[at, part + j:part + j + 1]).astype(BF16)

    def attend(p, e, j):
        slot = lax.rem(p, 2) * 2 + e
        for copy in cache_copies(p, e):
            copy.wait()
        b = p * 2 + e
        q = qall[p].reshape(rows, qall.shape[-1])
        cache = cbuf[slot]
        s = lax.dot_general(q[:, e * lat:(e + 1) * lat], cache, (((1,), (1,)), ((), ())), preferred_element_type=F32)
        s += jnp.dot(q[:, 2 * lat:], kbuf[slot], preferred_element_type=F32)
        token = lax.rem(lax.broadcasted_iota(jnp.int32, (rows, 1), 0), q_len)
        first = lax.axis_index("seq") * local_len
        positions = lax.broadcasted_iota(jnp.int32, (1, local_len), 1)
        visible = positions <= (token + (lens_ref[b] - first))
        s = jnp.where(visible, s * (scale * math.log2(math.e)), FILL)
        m = jnp.max(s, axis=1, keepdims=True)
        w = jnp.exp2(s - m)
        l = jnp.sum(w, axis=1, keepdims=True)
        o = jnp.dot(w.astype(BF16), cache, preferred_element_type=F32)
        obuf[b] = o.reshape(CORES, side, side, block, lat)
        r = j * 2 + e
        lane = lax.broadcasted_iota(jnp.int32, stat.shape, 1)
        at = (r // part) * 2 * part + lax.rem(r, part)
        stat[...] = jnp.where(lane == at, m, jnp.where(lane == at + part, l, stat[...]))

    for i in range(1, 7):
        both(gather, 0, lambda g: g.step(i))

    def chunk_body(k, carry):
        more, done = k + 1 < n_chunks, k >= 1

        @pl.when(more)
        def _():
            both(gather, k + 1, lambda g: g.step(1))

        def pair_body(j, carry):
            p = k * pairs + j
            for e in range(2):
                attend(p, e, j)

            @pl.when(p + 2 < n_pairs)
            def _():
                fetch(p + 2)

            for i in range(pairs):
                @pl.when(more & (j == i))
                def _():
                    if i < pairs - 1:
                        both(gather, k + 1, lambda g: g.step(i + 2))
                    else:
                        for n in range(pairs + 1, 7):
                            both(gather, k + 1, lambda g: g.step(n))

                @pl.when(done & (j == i))
                def _():
                    scatter_step(k - 1, i)
                    if i == pairs - 1:
                        scatter_step(k - 1, i + 1)
            return carry

        lax.fori_loop(0, pairs, pair_body, 0)
        pair_start(k)
        return carry

    lax.fori_loop(0, n_chunks, chunk_body, 0)
    for i in range(5):
        scatter_step(n_chunks - 1, i)

    def drain(k, carry):
        both(gather, k, lambda g: g.drain())
        both(scatter, k, lambda sc: sc.drain())
        for copy in pair_copies(k):
            copy.wait_send()
        return carry

    lax.fori_loop(0, n_chunks, drain, 0)


def attention(side, lens, q, ckv, krt, q_len, scale, chunk):
    batch, local_len, lat = ckv.shape
    rope = krt.shape[1]
    block = q.shape[1]
    lanes = side * side * block
    n = batch // chunk
    part, half = chunk // 2, chunk // 4
    dma = pltpu.SemaphoreType.DMA
    scratch = [
        pltpu.VMEM((batch // 2, CORES, side, side, block, q.shape[2]), BF16),
        pltpu.VMEM((batch, CORES, side, side, block, lat), F32),
        pltpu.VMEM((4, local_len, lat), BF16),
        pltpu.VMEM((4, 2 * rope, local_len), BF16),
        pltpu.VMEM((CORES * lanes, 128), F32),
        pltpu.VMEM((n, CORES, 2, 2 * part, lanes), F32),
        pltpu.VMEM((n, 2, 2 * part, lanes), F32),
        pltpu.VMEM((n, 2, SCATTER_MSGS, 2 * part, lanes), F32),
        pltpu.VMEM((n, 2, SCATTER_MSGS, 2 * part, lanes), F32),
        pltpu.VMEM((n, 2, 2 * part, lanes), F32),
        pltpu.VMEM((lanes, 128), F32),
        pltpu.VMEM((n, chunk, side, side, block, lat), F32),
        pltpu.VMEM((n, 2, 2, half, side, block, lat), F32),
        pltpu.VMEM((n, 2, 2, part, side, block, lat), F32),
        pltpu.VMEM((n, 2, 2, half, block, lat), F32),
        pltpu.VMEM((n, 2, 2, part, block, lat), F32),
        dma((n, 2, GATHER_MSGS)), dma((n, 2, GATHER_MSGS)),
        dma((n, 2, 2 * SCATTER_MSGS)), dma((n, 2, 2 * SCATTER_MSGS)),
        dma((n, 2)), dma((n, 2)), dma((4,)), dma((4,)),
    ]
    return pl.pallas_call(
        functools.partial(attention_kernel, (side, chunk, q_len, scale)),
        out_shape=jax.ShapeDtypeStruct((batch, block, lat), BF16),
        in_specs=[pl.BlockSpec(memory_space=pltpu.SMEM), pl.BlockSpec(memory_space=pltpu.VMEM),
                  pl.BlockSpec(memory_space=pl.ANY), pl.BlockSpec(memory_space=pl.ANY)],
        out_specs=pl.BlockSpec(memory_space=pltpu.VMEM),
        scratch_shapes=scratch,
        compiler_params=pltpu.CompilerParams(collective_id=0, has_side_effects=True, vmem_limit_bytes=VMEM_BYTES),
        name="attend_rings",
    )(lens, q, ckv, krt)


def output_kernel(side, ol_ref, wuv_ref, wo_ref, hid_ref, out_ref, y_buf, wo_buf, hid_buf, pair_land, far1, near1, far2, near2,
                  ssend, srecv, gsend, grecv, psend, precv, lsem):
    place = Place(side)
    core = place.core
    heads, _, value = wuv_ref.shape
    rb, width = y_buf.shape[2], y_buf.shape[3]
    mine = width // CORES
    part, half = mine // 2, mine // 4
    tiles = 4
    tile = mine // tiles
    n_rows = ol_ref.shape[0]
    tokens = hid_ref.shape[1]
    owned = rb // tokens

    wo_copy = pltpu.make_async_copy(wo_ref, wo_buf, lsem.at[0])
    wo_copy.start()
    col0 = pl.multiple_of(core * mine, 128)
    spot = place.y * side + place.x
    hid_copy = pltpu.make_async_copy(hid_ref.at[pl.ds(spot * owned, owned), :, pl.ds(col0, mine)], hid_buf, lsem.at[1])
    hid_copy.start()
    place.barrier()

    values = jnp.concatenate([wuv_ref[h] for h in range(heads)], axis=1)
    ov = jnp.dot(ol_ref[...], values, preferred_element_type=F32)
    row_head = lax.rem(lax.broadcasted_iota(jnp.int32, ov.shape, 0) // tokens, heads)
    col_head = lax.broadcasted_iota(jnp.int32, ov.shape, 1) // value
    ov = jnp.where(row_head == col_head, ov, 0.0).astype(BF16)
    shape = (n_rows // heads, n_rows)
    to = lax.broadcasted_iota(jnp.int32, shape, 0)
    frm = lax.broadcasted_iota(jnp.int32, shape, 1)
    same = (to // tokens == frm // (tokens * heads)) & (lax.rem(to, tokens) == lax.rem(frm, tokens))
    ov = jnp.dot(same.astype(F32).astype(BF16), ov, preferred_element_type=F32).astype(BF16)
    wo_copy.wait()

    def columns(c, t):
        return pl.ds(pl.multiple_of(c * mine + t * tile, 128), tile)

    def compute(c, t):
        y = jnp.dot(ov, wo_buf[:, columns(c, t)], preferred_element_type=F32)
        y_buf[:, :, :, columns(c, t)] = y.reshape(side, side, rb, tile)

    def pair_copy(t, arriving=False):
        there = pair_land.at[t]
        src = there if arriving else y_buf.at[:, :, :, columns(1 - core, t)]
        return remote(src, there, psend.at[t], precv.at[t], place.sibling())

    for t in range(tiles):
        compute(1 - core, t)
        pair_copy(t).start()
    for t in range(tiles):
        compute(core, t)
        pair_copy(t, arriving=True).wait_recv()
        y_buf[:, :, :, columns(core, t)] += pair_land[t]

    def cols(plane, h, c):
        lo, n = (0, part) if h is None else (h * half, half)
        return pl.ds(pl.multiple_of(c * mine + plane * part + lo, 128), n)

    def scatter(plane):
        def view(h, f, s):
            s = pl.ds(0, side) if s is None else s
            y, x = place.yx(plane, f, s)
            return y_buf.at[y, x, :, cols(plane, h, core)]

        def landing(msg):
            return {0: far1, 1: near1, 2: far2, 3: near2}[msg // 2].at[plane, msg % 2]

        def merge(h, f, s, msg):
            y, x = place.yx(plane, f, pl.ds(0, side) if s is None else s)
            y_buf[y, x, :, cols(plane, h, core)] += landing(msg)[...]

        return Scatter(place, plane, view, landing, merge, lambda m: None, lambda m: ssend.at[plane, m],
                       lambda m: srecv.at[plane, m])

    scs = [scatter(plane) for plane in range(2)]
    for sc in scs:
        sc.start(0, 1)
    for msg in (0, 1):
        for sc in scs:
            sc.take(msg)
            sc.start(msg + 2)
    for sc in scs:
        sc.take(2)
        sc.take(3)
        sc.start(4, 5)
    for msg in (4, 5):
        for sc in scs:
            sc.take(msg)
            sc.start(msg + 2)
    for sc in scs:
        sc.take(6)
        sc.take(7)
    hid_copy.wait()
    own = pl.ds(col0, mine)
    total = y_buf[place.y, place.x, :, own] + hid_buf[...].astype(F32).reshape(rb, mine)
    out_ref[place.y, place.x, :, own] = total.astype(BF16)

    def gather(plane):
        def view(c, h, f, s):
            f = pl.ds(0, side) if f is None else f
            y, x = place.yx(plane, f, s)
            return out_ref.at[y, x, :, cols(plane, h, c)]

        own = view(core, None, place.first[plane], place.second[plane])
        return Gather(place, plane, view, own, lambda m: gsend.at[plane, m], lambda m: grecv.at[plane, m])

    gs = [gather(plane) for plane in range(2)]
    for i in range(1, 7):
        for g in gs:
            g.step(i)
    for g in gs:
        g.drain()
    for sc in scs:
        sc.drain()
    for t in range(tiles):
        pair_copy(t).wait_send()


def output(side, ol, w_uv, wo, hidden):
    batch, tokens, width = hidden.shape
    rb = batch * tokens // (side * side)
    mine = width // CORES
    dma = pltpu.SemaphoreType.DMA
    return pl.pallas_call(
        functools.partial(output_kernel, side),
        out_shape=jax.ShapeDtypeStruct((side, side, rb, width), BF16),
        in_specs=[pl.BlockSpec(memory_space=pltpu.VMEM), pl.BlockSpec(memory_space=pltpu.VMEM),
                  pl.BlockSpec(memory_space=pl.ANY), pl.BlockSpec(memory_space=pl.ANY)],
        out_specs=pl.BlockSpec(memory_space=pltpu.VMEM),
        scratch_shapes=[
            pltpu.VMEM((side, side, rb, width), F32),
            pltpu.VMEM(wo.shape, BF16),
            pltpu.VMEM((rb // tokens, tokens, mine), BF16),
            pltpu.VMEM((4, side, side, rb, mine // 4), F32),
            pltpu.VMEM((2, 2, side, rb, mine // 4), F32),
            pltpu.VMEM((2, 2, side, rb, mine // 2), F32),
            pltpu.VMEM((2, 2, rb, mine // 4), F32),
            pltpu.VMEM((2, 2, rb, mine // 2), F32),
            dma((2, SCATTER_MSGS)), dma((2, SCATTER_MSGS)), dma((2, GATHER_MSGS)), dma((2, GATHER_MSGS)),
            dma((4,)), dma((4,)), dma((2,)),
        ],
        compiler_params=pltpu.CompilerParams(collective_id=1, has_side_effects=True, vmem_limit_bytes=VMEM_BYTES),
        name="project_rings",
    )(ol, w_uv, wo, hidden)


def solution(mesh):
    side = math.isqrt(mesh.shape["seq"] // CORES)

    def local_step(hidden, cache_lens, c_kv, k_r, w_uq, w_qr, w_uk, w_uv, w_o):
        batch, tokens, width = hidden.shape
        heads, lat = w_uk.shape[0], w_uk.shape[2]
        rope = w_qr.shape[2]
        block = heads * tokens
        scale = (w_uq.shape[2] + rope) ** -0.5
        q_nope = jnp.einsum("cre,eil->cril", hidden, w_uq, preferred_element_type=F32).astype(BF16)
        q_rope = jnp.einsum("cre,eis->cris", hidden, w_qr, preferred_element_type=F32).astype(BF16)
        q_lat = jnp.einsum("bqhk,hkc->bqhc", q_nope, w_uk, preferred_element_type=F32).astype(BF16)
        lat_pairs = q_lat.reshape(batch // 2, 2, tokens, heads, lat).transpose(0, 3, 2, 1, 4).reshape(batch // 2, block, 2 * lat)
        rope_pairs = q_rope.reshape(batch // 2, 2, tokens, heads, rope).transpose(0, 3, 2, 1, 4).reshape(batch // 2, block, 2 * rope)
        q = jnp.concatenate([lat_pairs, rope_pairs], axis=2)
        ol = attention(side, cache_lens, q, c_kv, k_r.transpose(0, 2, 1), tokens, scale, batch // 4)
        out = output(side, ol.reshape(batch * block, lat), w_uv, w_o.reshape(-1, width), hidden)
        return out.reshape(batch, tokens, width)

    specs_in = (P("batch", None, None), P("batch"), P("batch", "seq", None), P("batch", "seq", None),
                P(None, "seq", None), P(None, "seq", None), P("seq", None, None), P("seq", None, None),
                P("seq", None, None))
    return jax.shard_map(local_step, mesh=mesh, in_specs=specs_in, out_specs=P("batch", None, None), check_vma=False)
```

```python
import functools
import math

import jax
import jax.numpy as jnp
from jax import lax
from jax.experimental import pallas as pl
from jax.experimental.pallas import tpu as pltpu
from jax.sharding import PartitionSpec as P

MESH = pl.DeviceIdType.MESH
F32, BF16 = jnp.float32, jnp.bfloat16
FILL = float(jnp.finfo(jnp.float32).min)
CORES = 2
VMEM_BYTES = 67_043_328
TOP = 4
GATHER_SKEW = 2


class Place:
    def __init__(self, side):
        me = lax.axis_index("seq")
        self.side = side
        self.core = lax.rem(me, CORES)
        chip = me // CORES
        self.x, self.y = lax.rem(chip, side), chip // side
        self.first, self.second = (self.x, self.y), (self.y, self.x)

    def wrap(self, i):
        return lax.rem(i + self.side, self.side)

    def yx(self, plane, f, s):
        return (s, f) if plane == 0 else (f, s)

    def device(self, plane, f, s, core=None):
        y, x = self.yx(plane, f, s)
        return (y * self.side + x) * CORES + (self.core if core is None else core)

    def sibling(self):
        return self.device(0, self.x, self.y, 1 - self.core)

    def along_first(self, plane, step):
        return self.device(plane, self.wrap(self.first[plane] + step), self.second[plane])

    def along_second(self, plane, step):
        return self.device(plane, self.first[plane], self.wrap(self.second[plane] + step))

    def barrier(self):
        barrier = pltpu.get_barrier_semaphore()
        peers = [self.sibling()] + [self.along_first(p, d) for p in range(2) for d in (1, -1)]
        for peer in peers:
            pl.semaphore_signal(barrier, inc=1, device_id={"seq": peer}, device_id_type=MESH)
        pl.semaphore_wait(barrier, len(peers))


def remote(src, dst, send, recv, device):
    return pltpu.make_async_remote_copy(src_ref=src, dst_ref=dst, send_sem=send, recv_sem=recv, device_id={"seq": device},
                                        device_id_type=MESH)


GATHER_MSGS = 12


class Gather:
    def __init__(self, place, plane, view, own, send, recv):
        self.place, self.plane, self.view, self.own, self.send, self.recv = place, plane, view, own, send, recv

    def copy(self, msg, arriving=False):
        pc, p = self.place, self.plane
        f, s, c = pc.first[p], pc.second[p], pc.core
        w = pc.wrap
        sent, got, target = {
            0: ((None, f, s), (None, w(f - 1), s), pc.along_first(p, 1)),
            1: ((None, f, s), (None, w(f + 1), s), pc.along_first(p, -1)),
            2: ((0, w(f - 1), s), (0, w(f - 2), s), pc.along_first(p, 1)),
            3: ((1, w(f + 1), s), (1, w(f + 2), s), pc.along_first(p, -1)),
            4: ((None, None, s), (None, None, w(s - 1)), pc.along_second(p, 1)),
            5: ((None, None, s), (None, None, w(s + 1)), pc.along_second(p, -1)),
            6: ((0, None, w(s - 1)), (0, None, w(s - 2)), pc.along_second(p, 1)),
            7: ((1, None, w(s + 1)), (1, None, w(s + 2)), pc.along_second(p, -1)),
            8: ((None, None, s),) * 2 + (pc.sibling(),),
            9: ((None, None, w(s - 1)),) * 2 + (pc.sibling(),),
            10: ((None, None, w(s + 1)),) * 2 + (pc.sibling(),),
            11: ((None, None, w(s + 2)),) * 2 + (pc.sibling(),),
        }[msg]
        if arriving:
            dst = self.view(1 - c if msg >= 8 else c, *got)
            src = dst
        else:
            dst = self.view(c, *sent)
            src = self.own if msg in (0, 1) else dst
        return remote(src, dst, self.send(msg), self.recv(msg), target)

    def start(self, *msgs):
        for msg in msgs:
            self.copy(msg).start()

    def wait(self, *msgs):
        for msg in msgs:
            self.copy(msg, arriving=True).wait_recv()

    def step(self, i):
        if i == 1:
            self.start(0, 1)
        elif i == 2:
            self.wait(0)
            self.start(2)
            self.wait(1)
            self.start(3)
        elif i == 3:
            self.wait(2, 3)
            self.start(4, 5, 8)
        elif i == 4:
            self.wait(4)
            self.start(6, 9)
            self.wait(5)
            self.start(7, 10)
        elif i == 5:
            self.wait(6, 7)
            self.start(11)
        elif i == 6:
            self.wait(8, 9, 10, 11)

    def drain(self):
        for msg in range(GATHER_MSGS):
            self.copy(msg).wait_send()


SCATTER_MSGS = 8


class Scatter:
    def __init__(self, place, plane, view, landing, merge, extra, send, recv):
        self.place, self.plane, self.view, self.landing = place, plane, view, landing
        self.merge, self.extra, self.send, self.recv = merge, extra, send, recv

    def plan(self, msg):
        pc, p = self.place, self.plane
        f, s = pc.first[p], pc.second[p]
        w = pc.wrap
        return {
            0: ((0, w(f + 2), None), pc.along_first(p, 1), (0, w(f + 1), None)),
            1: ((1, w(f + 2), None), pc.along_first(p, -1), (1, w(f - 1), None)),
            2: ((None, w(f + 1), None), pc.along_first(p, 1), (None, f, None)),
            3: ((None, w(f - 1), None), pc.along_first(p, -1), (None, f, None)),
            4: ((0, f, w(s + 2)), pc.along_second(p, 1), (0, f, w(s + 1))),
            5: ((1, f, w(s + 2)), pc.along_second(p, -1), (1, f, w(s - 1))),
            6: ((None, f, w(s + 1)), pc.along_second(p, 1), (None, f, s)),
            7: ((None, f, w(s - 1)), pc.along_second(p, -1), (None, f, s)),
        }[msg]

    def copies(self, msg, arriving=False):
        sent, target, _ = self.plan(msg)
        dst = self.landing(msg)
        out = [remote(dst if arriving else self.view(*sent), dst, self.send(msg), self.recv(msg), target)]
        extra = self.extra(msg)
        if extra is not None:
            src, dst = extra
            i = msg + SCATTER_MSGS
            out.append(remote(dst if arriving else src, dst, self.send(i), self.recv(i), target))
        return out

    def start(self, *msgs):
        for msg in msgs:
            for copy in self.copies(msg):
                copy.start()

    def arrive(self, *msgs):
        for msg in msgs:
            for copy in self.copies(msg, arriving=True):
                copy.wait_recv()

    def take(self, msg):
        self.arrive(msg)
        self.merge(*self.plan(msg)[2], msg)

    def drain(self):
        for msg in range(SCATTER_MSGS):
            for copy in self.copies(msg):
                copy.wait_send()


def attention_kernel(cfg, lens_ref, q_ref, ckv_ref, krt_ref, o_ref, qall, obuf, cbuf, kbuf, stat, xt, tcur, tsend, tland, tpair,
                     factor, pair_land, far1, near1, far2, near2, gsend, grecv, ssend, srecv, psend, precv, csem, ksem):
    side, chunk, gather_pairs, q_len, scale = cfg
    place = Place(side)
    core = place.core
    batch, lat = ckv_ref.shape[0], ckv_ref.shape[2]
    rope, local_len = krt_ref.shape[1], krt_ref.shape[2]
    block = q_ref.shape[1]
    rows = CORES * side * side * block
    lanes = side * side * block
    n_pairs = batch // 2
    n_gather = n_pairs // gather_pairs
    n_chunks = batch // chunk
    pairs = chunk // 2
    part = chunk // 2
    half = part // 2

    def cache_copies(p, e):
        slot = lax.rem(p, 2) * 2 + e
        row = p * 2 + e
        return (pltpu.make_async_copy(ckv_ref.at[row], cbuf.at[slot], csem.at[slot]),
                pltpu.make_async_copy(krt_ref.at[row], kbuf.at[slot, pl.ds(e * rope, rope)], ksem.at[slot]))

    def fetch(p):
        for e in range(2):
            for copy in cache_copies(p, e):
                copy.start()

    for e in range(2):
        for i in range(2):
            kbuf[i * 2 + e, pl.ds((1 - e) * rope, rope)] = jnp.zeros((rope, local_len), BF16)
    fetch(0)
    fetch(1)

    for p in range(n_pairs):
        qall[p, core, place.y, place.x] = q_ref[p]
    stat[...] = jnp.zeros_like(stat)
    place.barrier()

    def gather(k, plane):
        base = k * gather_pairs + plane * (gather_pairs // 2)

        def view(c, h, f, s):
            if h is None:
                at = pl.ds(base, gather_pairs // 2)
            else:
                at = pl.ds(base + h * (gather_pairs // 4), gather_pairs // 4)
            f = pl.ds(0, side) if f is None else f
            y, x = place.yx(plane, f, s)
            return qall.at[at, c, y, x]

        return Gather(place, plane, view, q_ref.at[pl.ds(base, gather_pairs // 2)], lambda m: gsend.at[k, plane, m],
                      lambda m: grecv.at[k, plane, m])

    def fold(k, tables, masks):
        exps = []
        for plane in range(2):
            ts = tables[plane]
            m = functools.reduce(jnp.maximum, ts)
            es = [jnp.exp2(t - m) for t in ts]
            top = lax.broadcasted_iota(jnp.int32, m.shape, 0) < TOP
            sums = functools.reduce(jnp.add, [t * pltpu.roll(e, TOP, 0) for t, e in zip(ts, es)])
            joined = jnp.where(top, m, sums)
            tcur[k, plane] = joined if masks is None else jnp.where(masks[plane], joined, ts[0])
            exps += es
        factor[:, 0:8 * len(exps)] = jnp.concatenate(exps, 0).T

    def factors(i, y, x, j, n):
        at = pl.ds(pl.multiple_of((y * side + x) * block, block), block)
        return [factor[at, 8 * (i * n + t) + j:8 * (i * n + t) + j + 1] for t in range(n)]

    def region(plane, lo, n, f, s):
        shape = (8, lanes)
        spots = lax.broadcasted_iota(jnp.int32, shape, 1) // block
        ys, xs = spots // side, lax.rem(spots, side)
        fs, ss = (xs, ys) if plane == 0 else (ys, xs)
        b = lax.rem(lax.broadcasted_iota(jnp.int32, shape, 0), TOP)
        mine = (fs == f) & (b >= lo) & (b < lo + n)
        return mine if s is None else mine & (ss == s)

    def scatter(k, plane):
        base = k * chunk + plane * part

        def span(h):
            return (0, part) if h is None else (h * half, half)

        def view(h, f, s):
            lo, n = span(h)
            s = pl.ds(0, side) if s is None else s
            y, x = place.yx(plane, f, s)
            return obuf.at[pl.ds(base + lo, n), core, y, x]

        def landing(msg):
            return {0: far1, 1: near1, 2: far2, 3: near2}[msg // 2].at[k, plane, msg % 2]

        def extra(msg):
            return tsend.at[k, plane, msg], tland.at[k, plane, msg]

        return Scatter(place, plane, view, landing, None, extra, lambda m: ssend.at[k, plane, m],
                       lambda m: srecv.at[k, plane, m])

    def merge_far(k, msgs):
        tables, masks, jobs = [], [], []
        for plane in range(2):
            sc = scatter(k, plane)
            ta = tcur[k, plane]
            tb, mask = ta, None
            for msg in msgs:
                h, f, s = sc.plan(msg)[2]
                here = region(plane, h * half, half, f, s)
                tb = jnp.where(here, tland[k, plane, msg], tb)
                mask = here if mask is None else mask | here
                jobs.append((plane, h * half, half, f, s, [sc.landing(msg)]))
            tables.append([ta, tb])
            masks.append(mask)
        fold(k, tables, masks)
        apply(k, jobs)

    def merge_near(k, msgs):
        tables, masks, jobs = [], [], []
        for plane in range(2):
            sc = scatter(k, plane)
            _, f, s = sc.plan(msgs[0])[2]
            tables.append([tcur[k, plane]] + [tland[k, plane, msg] for msg in msgs])
            masks.append(region(plane, 0, part, f, s))
            jobs.append((plane, 0, part, f, s, [sc.landing(msg) for msg in msgs]))
        fold(k, tables, masks)
        apply(k, jobs)

    def apply(k, jobs):
        for plane, lo, n, f, s, lands in jobs:
            for j in range(n):
                b = k * chunk + plane * part + lo + j
                for i in range(side if s is None else 1):
                    y, x = place.yx(plane, f, i if s is None else s)
                    fs = factors(plane, y, x, lo + j, 1 + len(lands))
                    total = obuf[b, core, y, x] * fs[0]
                    for land, fac in zip(lands, fs[1:]):
                        total += (land[j, i] if s is None else land[j]) * fac
                    obuf[b, core, y, x] = total

    def both(make, k, act):
        for plane in range(2):
            act(make(k, plane))

    def snap(sc, k, *msgs):
        for msg in msgs:
            tsend[k, sc.plane, msg] = tcur[k, sc.plane]
        sc.start(*msgs)

    def pair_copies(k, arriving=False):
        there = pair_land.at[k]
        src = there if arriving else obuf.at[pl.ds(k * chunk, chunk), 1 - core]
        tables = tpair.at[k]
        tsrc = tables if arriving else xt.at[k, 1 - core]
        return (remote(src, there, psend.at[k, 0], precv.at[k, 0], place.sibling()),
                remote(tsrc, tables, psend.at[k, 1], precv.at[k, 1], place.sibling()))

    def pair_start(k):
        t = stat[...].T
        for c in range(CORES):
            for plane in range(2):
                xt[k, c, plane] = t[plane * 8:(plane + 1) * 8, c * lanes:(c + 1) * lanes]
        for copy in pair_copies(k):
            copy.start()

    def pair_merge(k):
        for copy in pair_copies(k, arriving=True):
            copy.wait_recv()
        fold(k, [[xt[k, core, plane], tpair[k, plane]] for plane in range(2)], None)

        def spot(i, carry):
            y, x = i // side, lax.rem(i, side)
            for plane in range(2):
                for j in range(part):
                    b = k * chunk + plane * part + j
                    fa, fb = factors(plane, y, x, j, 2)
                    obuf[b, core, y, x] = obuf[b, core, y, x] * fa + pair_land[k, plane * part + j, y, x] * fb
            return carry

        lax.fori_loop(0, side * side, spot, 0)

    def scatter_step(k, i):
        if i == 0:
            pair_merge(k)
            both(scatter, k, lambda sc: snap(sc, k, 0, 1))
            return
        msgs = (2 * i - 2, 2 * i - 1)
        both(scatter, k, lambda sc: sc.arrive(*msgs))
        (merge_far if i in (1, 3) else merge_near)(k, msgs)
        if i < 4:
            both(scatter, k, lambda sc: snap(sc, k, 2 * i, 2 * i + 1))
            return
        factor[:, 0:16] = jnp.concatenate([tcur[k, plane] for plane in range(2)], 0).T
        for plane in range(2):
            for j in range(part):
                b = k * chunk + plane * part + j
                l = factors(plane, place.y, place.x, TOP + j, 1)[0]
                o_ref[b] = (obuf[b, core, place.y, place.x] / l).astype(BF16)

    def attend(p, e):
        slot = lax.rem(p, 2) * 2 + e
        for copy in cache_copies(p, e):
            copy.wait()
        b = p * 2 + e
        q = qall[p].reshape(rows, qall.shape[-1])
        cache = cbuf[slot]
        s = lax.dot_general(q[:, e * lat:(e + 1) * lat], cache, (((1,), (1,)), ((), ())), preferred_element_type=F32)
        s += jnp.dot(q[:, 2 * lat:], kbuf[slot], preferred_element_type=F32)
        token = lax.rem(lax.broadcasted_iota(jnp.int32, (rows, 1), 0), q_len)
        first = lax.axis_index("seq") * local_len
        positions = lax.broadcasted_iota(jnp.int32, (1, local_len), 1)
        visible = positions <= (token + (lens_ref[b] - first))
        s = jnp.where(visible, s * (scale * math.log2(math.e)), FILL)
        m = jnp.max(s, axis=1, keepdims=True)
        w = jnp.exp2(s - m)
        l = jnp.sum(w, axis=1, keepdims=True)
        o = jnp.dot(w.astype(BF16), cache, preferred_element_type=F32)
        obuf[b] = o.reshape(CORES, side, side, block, lat)
        r = lax.rem(b, chunk)
        lane = lax.broadcasted_iota(jnp.int32, stat.shape, 1)
        at = (r // part) * 8 + lax.rem(r, part)
        stat[...] = jnp.where(lane == at, m, jnp.where(lane == at + TOP, l, stat[...]))

    last = 6 + GATHER_SKEW * (n_gather - 1)
    turns = [[(g, turn - GATHER_SKEW * g) for g in range(n_gather) if 1 <= turn - GATHER_SKEW * g <= 6]
             for turn in range(last + 1)]
    for turn in turns[:7]:
        for g, i in turn:
            both(gather, g, lambda ga: ga.step(i))

    def slot(h, carry):
        @pl.when(h < n_pairs)
        def _():
            for e in range(2):
                attend(h, e)

        @pl.when(h + 2 < n_pairs)
        def _():
            fetch(h + 2)

        for late, turn in enumerate(turns[7:]):
            @pl.when(h == late)
            def _():
                for g, i in turn:
                    both(gather, g, lambda ga: ga.step(i))

        for i in reversed(range(5)):
            k = (h - i) // pairs - 1

            @pl.when((h >= i + pairs) & (lax.rem(h + pairs * 5 - i, pairs) == 0) & (k < n_chunks))
            def _():
                scatter_step(k, i)

        @pl.when((h < n_pairs) & (lax.rem(h, pairs) == pairs - 1))
        def _():
            pair_start(h // pairs)

        return carry

    lax.fori_loop(0, n_pairs + 5, slot, 0)

    def drain_gather(k, carry):
        both(gather, k, lambda g: g.drain())
        return carry

    def drain(k, carry):
        both(scatter, k, lambda sc: sc.drain())
        for copy in pair_copies(k):
            copy.wait_send()
        return carry

    lax.fori_loop(0, n_gather, drain_gather, 0)
    lax.fori_loop(0, n_chunks, drain, 0)


def attention(side, lens, q, ckv, krt, q_len, scale, chunk, gather_pairs):
    batch, local_len, lat = ckv.shape
    rope = krt.shape[1]
    block = q.shape[1]
    lanes = side * side * block
    n = batch // chunk
    n_gather = batch // 2 // gather_pairs
    part, half = chunk // 2, chunk // 4
    dma = pltpu.SemaphoreType.DMA
    scratch = [
        pltpu.VMEM((batch // 2, CORES, side, side, block, q.shape[2]), BF16),
        pltpu.VMEM((batch, CORES, side, side, block, lat), F32),
        pltpu.VMEM((4, local_len, lat), BF16),
        pltpu.VMEM((4, 2 * rope, local_len), BF16),
        pltpu.VMEM((CORES * lanes, 128), F32),
        pltpu.VMEM((n, CORES, 2, 8, lanes), F32),
        pltpu.VMEM((n, 2, 8, lanes), F32),
        pltpu.VMEM((n, 2, SCATTER_MSGS, 8, lanes), F32),
        pltpu.VMEM((n, 2, SCATTER_MSGS, 8, lanes), F32),
        pltpu.VMEM((n, 2, 8, lanes), F32),
        pltpu.VMEM((lanes, 128), F32),
        pltpu.VMEM((n, chunk, side, side, block, lat), F32),
        pltpu.VMEM((n, 2, 2, half, side, block, lat), F32),
        pltpu.VMEM((n, 2, 2, part, side, block, lat), F32),
        pltpu.VMEM((n, 2, 2, half, block, lat), F32),
        pltpu.VMEM((n, 2, 2, part, block, lat), F32),
        dma((n_gather, 2, GATHER_MSGS)), dma((n_gather, 2, GATHER_MSGS)),
        dma((n, 2, 2 * SCATTER_MSGS)), dma((n, 2, 2 * SCATTER_MSGS)),
        dma((n, 2)), dma((n, 2)), dma((4,)), dma((4,)),
    ]
    return pl.pallas_call(
        functools.partial(attention_kernel, (side, chunk, gather_pairs, q_len, scale)),
        out_shape=jax.ShapeDtypeStruct((batch, block, lat), BF16),
        in_specs=[pl.BlockSpec(memory_space=pltpu.SMEM), pl.BlockSpec(memory_space=pltpu.VMEM),
                  pl.BlockSpec(memory_space=pl.ANY), pl.BlockSpec(memory_space=pl.ANY)],
        out_specs=pl.BlockSpec(memory_space=pltpu.VMEM),
        scratch_shapes=scratch,
        compiler_params=pltpu.CompilerParams(collective_id=0, has_side_effects=True, vmem_limit_bytes=VMEM_BYTES),
        name="attend_rings",
    )(lens, q, ckv, krt)


def output_kernel(side, ol_ref, wuv_ref, wo_ref, hid_ref, out_ref, y_buf, wo_buf, hid_buf, pair_land, far1, near1, far2, near2,
                  ssend, srecv, gsend, grecv, psend, precv, lsem):
    place = Place(side)
    core = place.core
    heads, _, value = wuv_ref.shape
    rb, width = y_buf.shape[2], y_buf.shape[3]
    mine = width // CORES
    part, half = mine // 2, mine // 4
    tiles = 4
    tile = mine // tiles
    n_rows = ol_ref.shape[0]
    tokens = hid_ref.shape[1]
    owned = rb // tokens

    wo_copy = pltpu.make_async_copy(wo_ref, wo_buf, lsem.at[0])
    wo_copy.start()
    col0 = pl.multiple_of(core * mine, 128)
    spot = place.y * side + place.x
    hid_copy = pltpu.make_async_copy(hid_ref.at[pl.ds(spot * owned, owned), :, pl.ds(col0, mine)], hid_buf, lsem.at[1])
    hid_copy.start()
    place.barrier()

    values = jnp.concatenate([wuv_ref[h] for h in range(heads)], axis=1)
    ov = jnp.dot(ol_ref[...], values, preferred_element_type=F32)
    row_head = lax.rem(lax.broadcasted_iota(jnp.int32, ov.shape, 0) // tokens, heads)
    col_head = lax.broadcasted_iota(jnp.int32, ov.shape, 1) // value
    ov = jnp.where(row_head == col_head, ov, 0.0).astype(BF16)
    shape = (n_rows // heads, n_rows)
    to = lax.broadcasted_iota(jnp.int32, shape, 0)
    frm = lax.broadcasted_iota(jnp.int32, shape, 1)
    same = (to // tokens == frm // (tokens * heads)) & (lax.rem(to, tokens) == lax.rem(frm, tokens))
    ov = jnp.dot(same.astype(F32).astype(BF16), ov, preferred_element_type=F32).astype(BF16)
    wo_copy.wait()

    def columns(c, t):
        return pl.ds(pl.multiple_of(c * mine + t * tile, 128), tile)

    def compute(c, t):
        y = jnp.dot(ov, wo_buf[:, columns(c, t)], preferred_element_type=F32)
        y_buf[:, :, :, columns(c, t)] = y.reshape(side, side, rb, tile)

    def pair_copy(t, arriving=False):
        there = pair_land.at[t]
        src = there if arriving else y_buf.at[:, :, :, columns(1 - core, t)]
        return remote(src, there, psend.at[t], precv.at[t], place.sibling())

    for t in range(tiles):
        compute(1 - core, t)
        pair_copy(t).start()
    for t in range(tiles):
        compute(core, t)
        pair_copy(t, arriving=True).wait_recv()
        y_buf[:, :, :, columns(core, t)] += pair_land[t]

    def cols(plane, h, c):
        lo, n = (0, part) if h is None else (h * half, half)
        return pl.ds(pl.multiple_of(c * mine + plane * part + lo, 128), n)

    def scatter(plane):
        def view(h, f, s):
            s = pl.ds(0, side) if s is None else s
            y, x = place.yx(plane, f, s)
            return y_buf.at[y, x, :, cols(plane, h, core)]

        def landing(msg):
            return {0: far1, 1: near1, 2: far2, 3: near2}[msg // 2].at[plane, msg % 2]

        def merge(h, f, s, msg):
            y, x = place.yx(plane, f, pl.ds(0, side) if s is None else s)
            y_buf[y, x, :, cols(plane, h, core)] += landing(msg)[...]

        return Scatter(place, plane, view, landing, merge, lambda m: None, lambda m: ssend.at[plane, m],
                       lambda m: srecv.at[plane, m])

    scs = [scatter(plane) for plane in range(2)]
    for sc in scs:
        sc.start(0, 1)
    for msg in (0, 1):
        for sc in scs:
            sc.take(msg)
            sc.start(msg + 2)
    for sc in scs:
        sc.take(2)
        sc.take(3)
        sc.start(4, 5)
    for msg in (4, 5):
        for sc in scs:
            sc.take(msg)
            sc.start(msg + 2)
    for sc in scs:
        sc.take(6)
        sc.take(7)
    hid_copy.wait()
    own = pl.ds(col0, mine)
    total = y_buf[place.y, place.x, :, own] + hid_buf[...].astype(F32).reshape(rb, mine)
    out_ref[place.y, place.x, :, own] = total.astype(BF16)

    def gather(plane):
        def view(c, h, f, s):
            f = pl.ds(0, side) if f is None else f
            y, x = place.yx(plane, f, s)
            return out_ref.at[y, x, :, cols(plane, h, c)]

        own = view(core, None, place.first[plane], place.second[plane])
        return Gather(place, plane, view, own, lambda m: gsend.at[plane, m], lambda m: grecv.at[plane, m])

    gs = [gather(plane) for plane in range(2)]
    for i in range(1, 7):
        for g in gs:
            g.step(i)
    for g in gs:
        g.drain()
    for sc in scs:
        sc.drain()
    for t in range(tiles):
        pair_copy(t).wait_send()


def output(side, ol, w_uv, wo, hidden):
    batch, tokens, width = hidden.shape
    rb = batch * tokens // (side * side)
    mine = width // CORES
    dma = pltpu.SemaphoreType.DMA
    return pl.pallas_call(
        functools.partial(output_kernel, side),
        out_shape=jax.ShapeDtypeStruct((side, side, rb, width), BF16),
        in_specs=[pl.BlockSpec(memory_space=pltpu.VMEM), pl.BlockSpec(memory_space=pltpu.VMEM),
                  pl.BlockSpec(memory_space=pl.ANY), pl.BlockSpec(memory_space=pl.ANY)],
        out_specs=pl.BlockSpec(memory_space=pltpu.VMEM),
        scratch_shapes=[
            pltpu.VMEM((side, side, rb, width), F32),
            pltpu.VMEM(wo.shape, BF16),
            pltpu.VMEM((rb // tokens, tokens, mine), BF16),
            pltpu.VMEM((4, side, side, rb, mine // 4), F32),
            pltpu.VMEM((2, 2, side, rb, mine // 4), F32),
            pltpu.VMEM((2, 2, side, rb, mine // 2), F32),
            pltpu.VMEM((2, 2, rb, mine // 4), F32),
            pltpu.VMEM((2, 2, rb, mine // 2), F32),
            dma((2, SCATTER_MSGS)), dma((2, SCATTER_MSGS)), dma((2, GATHER_MSGS)), dma((2, GATHER_MSGS)),
            dma((4,)), dma((4,)), dma((2,)),
        ],
        compiler_params=pltpu.CompilerParams(collective_id=1, has_side_effects=True, vmem_limit_bytes=VMEM_BYTES),
        name="project_rings",
    )(ol, w_uv, wo, hidden)


def solution(mesh):
    side = math.isqrt(mesh.shape["seq"] // CORES)

    def local_step(hidden, cache_lens, c_kv, k_r, w_uq, w_qr, w_uk, w_uv, w_o):
        batch, tokens, width = hidden.shape
        heads, lat = w_uk.shape[0], w_uk.shape[2]
        rope = w_qr.shape[2]
        block = heads * tokens
        scale = (w_uq.shape[2] + rope) ** -0.5
        q_nope = jnp.einsum("cre,eil->cril", hidden, w_uq, preferred_element_type=F32).astype(BF16)
        q_rope = jnp.einsum("cre,eis->cris", hidden, w_qr, preferred_element_type=F32).astype(BF16)
        q_lat = jnp.einsum("bqhk,hkc->bqhc", q_nope, w_uk, preferred_element_type=F32).astype(BF16)
        lat_pairs = q_lat.reshape(batch // 2, 2, tokens, heads, lat).transpose(0, 3, 2, 1, 4).reshape(batch // 2, block, 2 * lat)
        rope_pairs = q_rope.reshape(batch // 2, 2, tokens, heads, rope).transpose(0, 3, 2, 1, 4).reshape(batch // 2, block, 2 * rope)
        q = jnp.concatenate([lat_pairs, rope_pairs], axis=2)
        ol = attention(side, cache_lens, q, c_kv, k_r.transpose(0, 2, 1), tokens, scale, batch // 8, batch // 8)
        out = output(side, ol.reshape(batch * block, lat), w_uv, w_o.reshape(-1, width), hidden)
        return out.reshape(batch, tokens, width)

    specs_in = (P("batch", None, None), P("batch"), P("batch", "seq", None), P("batch", "seq", None),
                P(None, "seq", None), P(None, "seq", None), P("seq", None, None), P("seq", None, None),
                P("seq", None, None))
    return jax.shard_map(local_step, mesh=mesh, in_specs=specs_in, out_specs=P("batch", None, None), check_vma=False)
```

```python
import functools
import math

import jax
import jax.numpy as jnp
from jax import lax
from jax.experimental import pallas as pl
from jax.experimental.pallas import tpu as pltpu
from jax.sharding import PartitionSpec as P

MESH = pl.DeviceIdType.MESH
F32, BF16 = jnp.float32, jnp.bfloat16
FILL = float(jnp.finfo(jnp.float32).min)
CORES = 2
VMEM_BYTES = 67_043_328
TOP = 4
GATHER_TURN = ((1, 2, 3, 4), (2, 3, 5, 6, 7, 8), (4, 5, 7, 9, 11, 12), (6, 7, 10, 12, 14, 16))
SLOT_TURN = 5
STEP_SLOT = (0, 3, 6, 8, 10)
GROUP = 8
PARTS = 2


class Place:
    def __init__(self, side):
        me = lax.axis_index("seq")
        self.side = side
        self.core = lax.rem(me, CORES)
        chip = me // CORES
        self.x, self.y = lax.rem(chip, side), chip // side
        self.first, self.second = (self.x, self.y), (self.y, self.x)

    def wrap(self, i):
        return lax.rem(i + self.side, self.side)

    def yx(self, plane, f, s):
        return (s, f) if plane == 0 else (f, s)

    def device(self, plane, f, s, core=None):
        y, x = self.yx(plane, f, s)
        return (y * self.side + x) * CORES + (self.core if core is None else core)

    def around(self, i):
        return self.wrap(i + 1), self.wrap(i - 1), self.wrap(i + 2)

    def sibling(self):
        return self.device(0, self.x, self.y, 1 - self.core)

    def barrier(self):
        barrier = pltpu.get_barrier_semaphore()
        peers = [self.sibling()] + [self.device(p, f, self.second[p]) for p in range(2) for f in self.around(self.first[p])]
        for peer in peers:
            pl.semaphore_signal(barrier, inc=1, device_id={"seq": peer}, device_id_type=MESH)
        pl.semaphore_wait(barrier, len(peers))


def remote(src, dst, send, recv, device):
    return pltpu.make_async_remote_copy(src_ref=src, dst_ref=dst, send_sem=send, recv_sem=recv, device_id={"seq": device},
                                        device_id_type=MESH)


ALL, LOW, HIGH = None, 0, 1
GATHER_MSGS, TWIN_MSG, RELAYED = 12, 8, (3, 7)
TWINS = ((8, 9, 10, 11), ())
RING_STEPS = ((((), (0, 1)),), (((0,), (2,)), ((1,), (3,))), (((2, 3), (4, 5, 8)),), (((4,), (6, 9)), ((5,), (7, 10))),
              (((6, 7), (11,)),), (TWINS,))
DIRECT_STEPS = ((((), (0, 1, 2)),), (((0, 1, 2), (4, 5, 6, 8)),), (((4,), (9,)), ((5,), (10,)), ((6,), (11,))), (TWINS,))


class Gather:
    def __init__(self, place, plane, view, own, send, recv, direct=False):
        self.place, self.plane, self.view, self.own, self.send, self.recv = place, plane, view, own, send, recv
        self.direct = direct

    def copy(self, msg, arriving=False):
        pc, p = self.place, self.plane
        f, s, c, twin = pc.first[p], pc.second[p], pc.core, pc.sibling()
        f_up, f_down, f_far = pc.around(f)
        s_up, s_down, s_far = pc.around(s)
        to_f_up, to_f_down, to_f_far = [pc.device(p, i, s) for i in (f_up, f_down, f_far)]
        to_s_up, to_s_down, to_s_far = [pc.device(p, f, i) for i in (s_up, s_down, s_far)]
        row = (ALL, ALL, s)
        plans = [
            ((ALL, f, s), (ALL, f_down, s), to_f_up),
            ((ALL, f, s), (ALL, f_up, s), to_f_down),
            ((LOW, f_down, s), (LOW, f_far, s), to_f_up),
            ((HIGH, f_up, s), (HIGH, f_far, s), to_f_down),
            (row, (ALL, ALL, s_down), to_s_up),
            (row, (ALL, ALL, s_up), to_s_down),
            ((LOW, ALL, s_down), (LOW, ALL, s_far), to_s_up),
            ((HIGH, ALL, s_up), (HIGH, ALL, s_far), to_s_down),
        ]
        plans += [((ALL, ALL, i), (ALL, ALL, i), twin) for i in (s, s_down, s_up, s_far)]
        if self.direct:
            plans[2] = ((ALL, f, s), (ALL, f_far, s), to_f_far)
            plans[6] = (row, (ALL, ALL, s_far), to_s_far)
        sent, got, target = plans[msg]
        if arriving:
            dst = self.view(1 - c if msg >= TWIN_MSG else c, *got)
            src = dst
        else:
            dst = self.view(c, *sent)
            src = self.own if sent == (ALL, f, s) else dst
        return remote(src, dst, self.send(msg), self.recv(msg), target)

    def start(self, *msgs):
        for msg in msgs:
            self.copy(msg).start()

    def wait(self, *msgs):
        for msg in msgs:
            self.copy(msg, arriving=True).wait_recv()

    def step(self, i):
        for waits, starts in (DIRECT_STEPS if self.direct else RING_STEPS)[i - 1]:
            self.wait(*waits)
            self.start(*starts)

    def drain(self):
        for msg in range(GATHER_MSGS):
            if not (self.direct and msg in RELAYED):
                self.copy(msg).wait_send()


SCATTER_MSGS = 8


class Scatter:
    def __init__(self, place, plane, view, landing, merge, extra, send, recv):
        self.place, self.plane, self.view, self.landing = place, plane, view, landing
        self.merge, self.extra, self.send, self.recv = merge, extra, send, recv

    def plan(self, msg):
        pc, p = self.place, self.plane
        f, s = pc.first[p], pc.second[p]
        f_up, f_down, f_far = pc.around(f)
        s_up, s_down, s_far = pc.around(s)
        to_f_up, to_f_down = [pc.device(p, i, s) for i in (f_up, f_down)]
        to_s_up, to_s_down = [pc.device(p, f, i) for i in (s_up, s_down)]
        return [
            ((LOW, f_far, ALL), to_f_up, (LOW, f_up, ALL)),
            ((HIGH, f_far, ALL), to_f_down, (HIGH, f_down, ALL)),
            ((ALL, f_up, ALL), to_f_up, (ALL, f, ALL)),
            ((ALL, f_down, ALL), to_f_down, (ALL, f, ALL)),
            ((LOW, f, s_far), to_s_up, (LOW, f, s_up)),
            ((HIGH, f, s_far), to_s_down, (HIGH, f, s_down)),
            ((ALL, f, s_up), to_s_up, (ALL, f, s)),
            ((ALL, f, s_down), to_s_down, (ALL, f, s)),
        ][msg]

    def copies(self, msg, arriving=False):
        sent, target, _ = self.plan(msg)
        dst = self.landing(msg)
        out = [remote(dst if arriving else self.view(*sent), dst, self.send(msg), self.recv(msg), target)]
        extra = self.extra(msg)
        if extra is not None:
            src, dst = extra
            i = msg + SCATTER_MSGS
            out.append(remote(dst if arriving else src, dst, self.send(i), self.recv(i), target))
        return out

    def start(self, *msgs):
        for msg in msgs:
            for copy in self.copies(msg):
                copy.start()

    def arrive(self, *msgs):
        for msg in msgs:
            for copy in self.copies(msg, arriving=True):
                copy.wait_recv()

    def take(self, msg):
        self.arrive(msg)
        self.merge(*self.plan(msg)[2], msg)

    def drain(self):
        for msg in range(SCATTER_MSGS):
            for copy in self.copies(msg):
                copy.wait_send()


def attention_kernel(cfg, lens_ref, q_ref, ckv_ref, krt_ref, o_ref, qall, obuf, cbuf, kbuf, stat, xt, tcur, tsend, tland, tpair,
                     factor, pair_land, far1, near1, far2, near2, gsend, grecv, ssend, srecv, psend, precv, csem, ksem):
    side, chunk, gather_pairs, q_len, scale = cfg
    place = Place(side)
    core = place.core
    batch, lat = ckv_ref.shape[0], ckv_ref.shape[2]
    rope, local_len = krt_ref.shape[1], krt_ref.shape[2]
    block = q_ref.shape[1]
    rows = CORES * side * side * block
    lanes = side * side * block
    n_pairs = batch // 2
    n_gather = n_pairs // gather_pairs
    n_chunks = batch // chunk
    pairs = chunk // 2
    part = chunk // 2
    half = part // 2

    def cache_copies(p, e):
        slot = lax.rem(p, 2) * 2 + e
        row = p * 2 + e
        return (pltpu.make_async_copy(ckv_ref.at[row], cbuf.at[slot], csem.at[slot]),
                pltpu.make_async_copy(krt_ref.at[row], kbuf.at[slot, pl.ds(e * rope, rope)], ksem.at[slot]))

    def fetch(p):
        for e in range(2):
            for copy in cache_copies(p, e):
                copy.start()

    for e in range(2):
        for i in range(2):
            kbuf[i * 2 + e, pl.ds((1 - e) * rope, rope)] = jnp.zeros((rope, local_len), BF16)
    fetch(0)
    fetch(1)

    for p in range(n_pairs):
        qall[p, core, place.y, place.x] = q_ref[p]
    stat[...] = jnp.zeros_like(stat)
    place.barrier()

    def gather(k, plane):
        base = k * gather_pairs + plane * (gather_pairs // 2)

        def view(c, h, f, s):
            if h is None:
                at = pl.ds(base, gather_pairs // 2)
            else:
                at = pl.ds(base + h * (gather_pairs // 4), gather_pairs // 4)
            f = pl.ds(0, side) if f is None else f
            y, x = place.yx(plane, f, s)
            return qall.at[at, c, y, x]

        return Gather(place, plane, view, q_ref.at[pl.ds(base, gather_pairs // 2)], lambda m: gsend.at[k, plane, m],
                      lambda m: grecv.at[k, plane, m], isinstance(k, int) and k == 0)

    def fold(k, tables, masks):
        exps = []
        for plane in range(2):
            ts = tables[plane]
            m = functools.reduce(jnp.maximum, ts)
            es = [jnp.exp2(t - m) for t in ts]
            top = lax.broadcasted_iota(jnp.int32, m.shape, 0) < TOP
            sums = functools.reduce(jnp.add, [t * pltpu.roll(e, TOP, 0) for t, e in zip(ts, es)])
            joined = jnp.where(top, m, sums)
            tcur[k, plane] = joined if masks is None else jnp.where(masks[plane], joined, ts[0])
            exps += es
        factor[:, 0:8 * len(exps)] = jnp.concatenate(exps, 0).T

    def factors(i, y, x, j, n):
        at = pl.ds(pl.multiple_of((y * side + x) * block, block), block)
        return [factor[at, 8 * (i * n + t) + j:8 * (i * n + t) + j + 1] for t in range(n)]

    def region(plane, lo, n, f, s):
        shape = (8, lanes)
        spots = lax.broadcasted_iota(jnp.int32, shape, 1) // block
        ys, xs = spots // side, lax.rem(spots, side)
        fs, ss = (xs, ys) if plane == 0 else (ys, xs)
        b = lax.rem(lax.broadcasted_iota(jnp.int32, shape, 0), TOP)
        mine = (fs == f) & (b >= lo) & (b < lo + n)
        return mine if s is None else mine & (ss == s)

    def scatter(k, plane):
        base = k * chunk + plane * part

        def span(h):
            return (0, part) if h is None else (h * half, half)

        def view(h, f, s):
            lo, n = span(h)
            s = pl.ds(0, side) if s is None else s
            y, x = place.yx(plane, f, s)
            return obuf.at[pl.ds(base + lo, n), core, y, x]

        def landing(msg):
            return {0: far1, 1: near1, 2: far2, 3: near2}[msg // 2].at[k, plane, msg % 2]

        def extra(msg):
            return tsend.at[k, plane, msg], tland.at[k, plane, msg]

        return Scatter(place, plane, view, landing, None, extra, lambda m: ssend.at[k, plane, m],
                       lambda m: srecv.at[k, plane, m])

    def merge_far(k, msgs):
        tables, masks, jobs = [], [], []
        for plane in range(2):
            sc = scatter(k, plane)
            ta = tcur[k, plane]
            tb, mask = ta, None
            for msg in msgs:
                h, f, s = sc.plan(msg)[2]
                here = region(plane, h * half, half, f, s)
                tb = jnp.where(here, tland[k, plane, msg], tb)
                mask = here if mask is None else mask | here
                jobs.append((plane, h * half, half, f, s, [sc.landing(msg)]))
            tables.append([ta, tb])
            masks.append(mask)
        fold(k, tables, masks)
        apply(k, jobs)

    def merge_near(k, msgs):
        tables, masks, jobs = [], [], []
        for plane in range(2):
            sc = scatter(k, plane)
            _, f, s = sc.plan(msgs[0])[2]
            tables.append([tcur[k, plane]] + [tland[k, plane, msg] for msg in msgs])
            masks.append(region(plane, 0, part, f, s))
            jobs.append((plane, 0, part, f, s, [sc.landing(msg) for msg in msgs]))
        fold(k, tables, masks)
        apply(k, jobs)

    def apply(k, jobs):
        blocks = [(plane, j, i, f, s, lo, lands) for plane, lo, n, f, s, lands in jobs for j in range(n)
                  for i in range(side if s is None else 1)]
        facs = []
        for plane, j, i, f, s, lo, lands in blocks:
            y, x = place.yx(plane, f, i if s is None else s)
            facs.append((y, x, factors(plane, y, x, lo + j, 1 + len(lands))))
        for g in range(0, len(blocks), GROUP):
            totals = []
            for (plane, j, i, f, s, lo, lands), (y, x, fs) in zip(blocks[g:g + GROUP], facs[g:g + GROUP]):
                b = k * chunk + plane * part + lo + j
                total = obuf[b, core, y, x] * fs[0]
                for land, fac in zip(lands, fs[1:]):
                    total += (land[j, i] if s is None else land[j]) * fac
                totals.append((b, y, x, total))
            for b, y, x, total in totals:
                obuf[b, core, y, x] = total

    def both(make, k, act):
        for plane in range(2):
            act(make(k, plane))

    def snap(sc, k, *msgs):
        for msg in msgs:
            tsend[k, sc.plane, msg] = tcur[k, sc.plane]
        sc.start(*msgs)

    def pair_copies(k, arriving=False):
        there = pair_land.at[k]
        src = there if arriving else obuf.at[pl.ds(k * chunk, chunk), 1 - core]
        tables = tpair.at[k]
        tsrc = tables if arriving else xt.at[k, 1 - core]
        return (remote(src, there, psend.at[k, 0], precv.at[k, 0], place.sibling()),
                remote(tsrc, tables, psend.at[k, 1], precv.at[k, 1], place.sibling()))

    def pair_start(k):
        t = stat[...].T
        for c in range(CORES):
            for plane in range(2):
                xt[k, c, plane] = t[plane * 8:(plane + 1) * 8, c * lanes:(c + 1) * lanes]
        for copy in pair_copies(k):
            copy.start()

    def pair_merge(k):
        for copy in pair_copies(k, arriving=True):
            copy.wait_recv()
        fold(k, [[xt[k, core, plane], tpair[k, plane]] for plane in range(2)], None)

        def spots(t, carry):
            facs, totals = {}, []
            spans = [(plane, j, x) for plane in range(2) for j in range(part) for x in range(side)]
            for plane, j, x in spans:
                facs[plane, j, x] = factors(plane, t, x, j, 2)
            for g in range(0, len(spans), GROUP):
                totals = []
                for plane, j, x in spans[g:g + GROUP]:
                    b = k * chunk + plane * part + j
                    fa, fb = facs[plane, j, x]
                    totals.append((b, x, obuf[b, core, t, x] * fa + pair_land[k, plane * part + j, t, x] * fb))
                for b, x, total in totals:
                    obuf[b, core, t, x] = total
            return carry

        lax.fori_loop(0, side, spots, 0)

    def scatter_step(k, i):
        if i == 0:
            pair_merge(k)
            both(scatter, k, lambda sc: snap(sc, k, 0, 1))
            return
        msgs = (2 * i - 2, 2 * i - 1)
        both(scatter, k, lambda sc: sc.arrive(*msgs))
        (merge_far if i in (1, 3) else merge_near)(k, msgs)
        if i < 4:
            both(scatter, k, lambda sc: snap(sc, k, 2 * i, 2 * i + 1))
            return
        factor[:, 0:16] = jnp.concatenate([tcur[k, plane] for plane in range(2)], 0).T
        for plane in range(2):
            for j in range(part):
                b = k * chunk + plane * part + j
                l = factors(plane, place.y, place.x, TOP + j, 1)[0]
                o_ref[b] = (obuf[b, core, place.y, place.x] / l).astype(BF16)

    def attend(p, e):
        slot = lax.rem(p, 2) * 2 + e
        for copy in cache_copies(p, e):
            copy.wait()
        b = p * 2 + e
        q = qall[p].reshape(rows, qall.shape[-1])
        cache = cbuf[slot]
        s = lax.dot_general(q[:, e * lat:(e + 1) * lat], cache, (((1,), (1,)), ((), ())), preferred_element_type=F32)
        s += jnp.dot(q[:, 2 * lat:], kbuf[slot], preferred_element_type=F32)
        token = lax.rem(lax.broadcasted_iota(jnp.int32, (rows, 1), 0), q_len)
        first = lax.axis_index("seq") * local_len
        positions = lax.broadcasted_iota(jnp.int32, (1, local_len), 1)
        visible = positions <= (token + (lens_ref[b] - first))
        s = jnp.where(visible, s * (scale * math.log2(math.e)), FILL)
        m = jnp.max(s, axis=1, keepdims=True)
        w = jnp.exp2(s - m)
        l = jnp.sum(w, axis=1, keepdims=True)
        o = jnp.dot(w.astype(BF16), cache, preferred_element_type=F32)
        obuf[b] = o.reshape(CORES, side, side, block, lat)
        r = lax.rem(b, chunk)
        lane = lax.broadcasted_iota(jnp.int32, stat.shape, 1)
        at = (r // part) * 8 + lax.rem(r, part)
        stat[...] = jnp.where(lane == at, m, jnp.where(lane == at + TOP, l, stat[...]))

    turns = [[(g, i + 1) for g in range(n_gather) for i, at in enumerate(GATHER_TURN[g]) if at == turn]
             for turn in range(max(map(max, GATHER_TURN)) + 1)]
    for turn in turns[:SLOT_TURN]:
        for g, i in turn:
            both(gather, g, lambda ga: ga.step(i))

    def slot(h, carry):
        @pl.when(h < n_pairs)
        def _():
            for e in range(2):
                attend(h, e)

        @pl.when(h + 2 < n_pairs)
        def _():
            fetch(h + 2)

        @pl.when((h < n_pairs) & (lax.rem(h, pairs) == pairs - 1))
        def _():
            pair_start(h // pairs)

        for late, turn in enumerate(turns[SLOT_TURN:]):
            @pl.when(h == late)
            def _():
                for g, i in turn:
                    both(gather, g, lambda ga: ga.step(i))

        for i in reversed(range(5)):
            since = h - STEP_SLOT[i]
            k = since // pairs - 1

            @pl.when((since >= pairs) & (lax.rem(since + pairs * 5, pairs) == 0) & (k < n_chunks))
            def _():
                scatter_step(k, i)

        return carry

    lax.fori_loop(0, n_pairs + STEP_SLOT[4] + 1, slot, 0)

    def drain_gather(k, carry):
        both(gather, k, lambda g: g.drain())
        return carry

    def drain(k, carry):
        both(scatter, k, lambda sc: sc.drain())
        for copy in pair_copies(k):
            copy.wait_send()
        return carry

    def drain_all():
        both(gather, 0, lambda g: g.drain())
        lax.fori_loop(1, n_gather, drain_gather, 0)
        lax.fori_loop(0, n_chunks, drain, 0)

    return drain_all


def step(side, lens, q, ckv, krt, w_uv, wo, hidden, q_len, scale, chunk, gather_pairs):
    batch, local_len, lat = ckv.shape
    rope = krt.shape[1]
    block = q.shape[1]
    lanes = side * side * block
    n = batch // chunk
    n_gather = batch // 2 // gather_pairs
    part, half = chunk // 2, chunk // 4
    dma = pltpu.SemaphoreType.DMA
    scratch = [
        pltpu.VMEM((batch // 2, CORES, side, side, block, q.shape[2]), BF16),
        pltpu.VMEM((batch, CORES, side, side, block, lat), F32),
        pltpu.VMEM((4, local_len, lat), BF16),
        pltpu.VMEM((4, 2 * rope, local_len), BF16),
        pltpu.VMEM((CORES * lanes, 128), F32),
        pltpu.VMEM((n, CORES, 2, 8, lanes), F32),
        pltpu.VMEM((n, 2, 8, lanes), F32),
        pltpu.VMEM((n, 2, SCATTER_MSGS, 8, lanes), F32),
        pltpu.VMEM((n, 2, SCATTER_MSGS, 8, lanes), F32),
        pltpu.VMEM((n, 2, 8, lanes), F32),
        pltpu.VMEM((lanes, 128), F32),
        pltpu.VMEM((n, chunk, side, side, block, lat), F32),
        pltpu.VMEM((n, 2, 2, half, side, block, lat), F32),
        pltpu.VMEM((n, 2, 2, part, side, block, lat), F32),
        pltpu.VMEM((n, 2, 2, half, block, lat), F32),
        pltpu.VMEM((n, 2, 2, part, block, lat), F32),
        dma((n_gather, 2, GATHER_MSGS)), dma((n_gather, 2, GATHER_MSGS)),
        dma((n, 2, 2 * SCATTER_MSGS)), dma((n, 2, 2 * SCATTER_MSGS)),
        dma((n, 2)), dma((n, 2)), dma((4,)), dma((4,)),
    ]
    tokens, width = hidden.shape[1:]
    rb = batch * tokens // (side * side)
    mine = width // CORES
    cols = mine // PARTS // 2
    far = cols - cols // 256 * 128
    out_scratch = [
        pltpu.VMEM((side, side, rb, width), F32),
        pltpu.VMEM(wo.shape, BF16),
        pltpu.VMEM((rb // tokens, tokens, mine), BF16),
        pltpu.VMEM((PARTS, 2, side, side, rb, cols), F32),
        pltpu.VMEM((PARTS, 2, 2, side, rb, far), F32),
        pltpu.VMEM((PARTS, 2, 2, side, rb, cols), F32),
        pltpu.VMEM((PARTS, 2, 2, rb, far), F32),
        pltpu.VMEM((PARTS, 2, 2, rb, cols), F32),
        dma((PARTS, 2, SCATTER_MSGS)), dma((PARTS, 2, SCATTER_MSGS)),
        dma((PARTS, 2, GATHER_MSGS)), dma((PARTS, 2, GATHER_MSGS)),
        dma((PARTS, 2)), dma((PARTS, 2)), dma((2,)),
    ]
    vmem, hbm = pl.BlockSpec(memory_space=pltpu.VMEM), pl.BlockSpec(memory_space=pl.ANY)
    return pl.pallas_call(
        functools.partial(whole_kernel, (side, chunk, gather_pairs, q_len, scale), len(scratch)),
        out_shape=jax.ShapeDtypeStruct((side, side, rb // tokens, tokens, width), BF16),
        in_specs=[pl.BlockSpec(memory_space=pltpu.SMEM), vmem, hbm, hbm, vmem, hbm, hbm],
        out_specs=vmem,
        scratch_shapes=[pltpu.VMEM((batch, block, lat), BF16)] + scratch + out_scratch,
        compiler_params=pltpu.CompilerParams(collective_id=0, has_side_effects=True, vmem_limit_bytes=VMEM_BYTES),
        name="latent_step",
    )(lens, q, ckv, krt, w_uv, wo, hidden)


def output_loads(place, wo_ref, hid_ref, wo_buf, hid_buf, lsem):
    owned, _, mine = hid_buf.shape
    spot = place.y * place.side + place.x
    cols = pl.ds(pl.multiple_of(place.core * mine, 128), mine)
    return (pltpu.make_async_copy(wo_ref, wo_buf, lsem.at[0]),
            pltpu.make_async_copy(hid_ref.at[pl.ds(spot * owned, owned), :, cols], hid_buf, lsem.at[1]))


def output_kernel(side, ol_ref, wuv_ref, wo_ref, hid_ref, out_ref, y_buf, wo_buf, hid_buf, pair_land, far1, near1, far2, near2,
                  ssend, srecv, gsend, grecv, psend, precv, lsem):
    place = Place(side)
    core = place.core
    heads, _, value = wuv_ref.shape
    rb, width = y_buf.shape[2], y_buf.shape[3]
    mine = width // CORES
    wide = mine // PARTS
    part = wide // 2
    half = part // 256 * 128
    n_rows = ol_ref.shape[0] * ol_ref.shape[1]
    tokens = hid_ref.shape[1]
    owned = rb // tokens

    wo_copy, hid_copy = output_loads(place, wo_ref, hid_ref, wo_buf, hid_buf, lsem)
    values = jnp.concatenate([wuv_ref[h] for h in range(heads)], axis=1)
    ov = jnp.dot(ol_ref[...].reshape(-1, ol_ref.shape[-1]), values, preferred_element_type=F32)
    row_head = lax.rem(lax.broadcasted_iota(jnp.int32, ov.shape, 0) // tokens, heads)
    col_head = lax.broadcasted_iota(jnp.int32, ov.shape, 1) // value
    ov = jnp.where(row_head == col_head, ov, 0.0).astype(BF16)
    shape = (n_rows // heads, n_rows)
    to = lax.broadcasted_iota(jnp.int32, shape, 0)
    frm = lax.broadcasted_iota(jnp.int32, shape, 1)
    same = (to // tokens == frm // (tokens * heads)) & (lax.rem(to, tokens) == lax.rem(frm, tokens))
    ov = jnp.dot(same.astype(F32).astype(BF16), ov, preferred_element_type=F32).astype(BF16)
    wo_copy.wait()

    def span(h):
        return {None: (0, part), 0: (0, half), 1: (half, part - half)}[h]

    def cols(q, plane, h, c):
        lo, n = span(h)
        return pl.ds(pl.multiple_of(c * mine + q * wide + plane * part + lo, 128), n)

    def compute(q, plane, c):
        at = cols(q, plane, None, c)
        y = jnp.dot(ov, wo_buf[:, at], preferred_element_type=F32)
        y_buf[:, :, :, at] = y.reshape(side, side, rb, part)

    def pair_copy(q, plane, arriving=False):
        there = pair_land.at[q, plane]
        src = there if arriving else y_buf.at[:, :, :, cols(q, plane, None, 1 - core)]
        return remote(src, there, psend.at[q, plane], precv.at[q, plane], place.sibling())

    def scatter(q, plane):
        def view(h, f, s):
            s = pl.ds(0, side) if s is None else s
            y, x = place.yx(plane, f, s)
            return y_buf.at[y, x, :, cols(q, plane, h, core)]

        def landing(msg):
            d = msg % 2
            n = span(d)[1]
            return {0: far1.at[q, plane, d, :, :, pl.ds(0, n)], 1: near1.at[q, plane, d],
                    2: far2.at[q, plane, d, :, pl.ds(0, n)], 3: near2.at[q, plane, d]}[msg // 2]

        def merge(h, f, s, msg):
            y, x = place.yx(plane, f, pl.ds(0, side) if s is None else s)
            y_buf[y, x, :, cols(q, plane, h, core)] += landing(msg)[...]

        return Scatter(place, plane, view, landing, merge, lambda m: None, lambda m: ssend.at[q, plane, m],
                       lambda m: srecv.at[q, plane, m])

    def gather(q, plane):
        def view(c, h, f, s):
            f = pl.ds(0, side) if f is None else f
            y, x = place.yx(plane, f, s)
            return out_ref.at[y, x, :, :, cols(q, plane, h, c)]

        own = view(core, None, place.first[plane], place.second[plane])
        return Gather(place, plane, view, own, lambda m: gsend.at[q, plane, m], lambda m: grecv.at[q, plane, m], True)

    scs = [[scatter(q, plane) for plane in range(2)] for q in range(PARTS)]
    gs = [[gather(q, plane) for plane in range(2)] for q in range(PARTS)]

    for q in range(PARTS):
        for plane in range(2):
            compute(q, plane, 1 - core)
            pair_copy(q, plane).start()
    for q in range(PARTS):
        for plane in range(2):
            compute(q, plane, core)
            pair_copy(q, plane, arriving=True).wait_recv()
            y_buf[:, :, :, cols(q, plane, None, core)] += pair_land[q, plane]
            scs[q][plane].start(0, 1)
    hid_copy.wait()
    for i in range(1, 5):
        for q in range(PARTS):
            for sc in scs[q]:
                for msg in (2 * i - 2, 2 * i - 1):
                    sc.take(msg)
                    if i in (1, 3):
                        sc.start(msg + 2)
                if i == 2:
                    sc.start(4, 5)
            if i == 4:
                own = pl.ds(pl.multiple_of(core * mine + q * wide, 128), wide)
                total = y_buf[place.y, place.x, :, own].reshape(owned, tokens, wide)
                total += hid_buf[:, :, q * wide:(q + 1) * wide].astype(F32)
                out_ref[place.y, place.x, :, :, own] = total.astype(BF16)
                for g in gs[q]:
                    g.step(1)
    for i in range(2, 5):
        for q in range(PARTS):
            for g in gs[q]:
                g.step(i)
    for q in range(PARTS):
        for plane in range(2):
            gs[q][plane].drain()
            scs[q][plane].drain()
            pair_copy(q, plane).wait_send()


def whole_kernel(cfg, n_scratch, lens_ref, q_ref, ckv_ref, krt_ref, wuv_ref, wo_ref, hid_ref, out_ref, ol_buf, *scratch):
    first, second = scratch[:n_scratch], scratch[n_scratch:]
    wo_buf, hid_buf, lsem = second[1], second[2], second[-1]
    for copy in output_loads(Place(cfg[0]), wo_ref, hid_ref, wo_buf, hid_buf, lsem):
        copy.start()
    drain = attention_kernel(cfg, lens_ref, q_ref, ckv_ref, krt_ref, ol_buf, *first)
    output_kernel(cfg[0], ol_buf, wuv_ref, wo_ref, hid_ref, out_ref, *second)
    drain()


def solution(mesh):
    side = math.isqrt(mesh.shape["seq"] // CORES)

    def local_step(hidden, cache_lens, c_kv, k_r, w_uq, w_qr, w_uk, w_uv, w_o):
        batch, tokens, width = hidden.shape
        heads, lat = w_uk.shape[0], w_uk.shape[2]
        rope = w_qr.shape[2]
        block = heads * tokens
        scale = (w_uq.shape[2] + rope) ** -0.5
        q_nope = jnp.einsum("cre,eil->cril", hidden, w_uq, preferred_element_type=F32).astype(BF16)
        q_rope = jnp.einsum("cre,eis->cris", hidden, w_qr, preferred_element_type=F32).astype(BF16)
        q_lat = jnp.einsum("bqhk,hkc->bqhc", q_nope, w_uk, preferred_element_type=F32).astype(BF16)
        def paired(v):
            v = v.reshape(batch // 2, 2, tokens, heads, -1).transpose(0, 3, 2, 1, 4)
            return v.reshape(batch // 2, block, -1)

        q = jnp.concatenate([paired(q_lat), paired(q_rope)], axis=2)
        out = step(side, cache_lens, q, c_kv, k_r.transpose(0, 2, 1), w_uv, w_o.reshape(-1, width), hidden, tokens, scale,
                   batch // 8, batch // 8)
        return out.reshape(batch, tokens, width)

    rows, heads, middle = P("batch"), P("seq"), P(None, "seq")
    cache = P("batch", "seq")
    specs_in = (rows, rows, cache, cache, middle, middle, heads, heads, heads)
    return jax.shard_map(local_step, mesh=mesh, in_specs=specs_in, out_specs=rows, check_vma=False)
```
